32 devices in a mesh: seq: 8 (over z, x), head: 4 (over y, core).
Axes of the slice: x: 2, y: 2, z: 4, core: 2. Of those that a mesh axis runs over, the one named last changes fastest.
Arguments:
- video_q: bfloat16 [1024, 4096], P(('seq', 'head')), may hold values from -200 to 200
- video_k: bfloat16 [1024, 4096], P(('seq', 'head')), may hold values from -6 to 6
- video_v: bfloat16 [1024, 4096], P(('seq', 'head')), may hold values from -6 to 6
- text_k: bfloat16 [512, 4096], P(None, 'head'), may hold values from -6 to 6
- text_v: bfloat16 [512, 4096], P(None, 'head'), may hold values from -6 to 6
- out_weight: bfloat16 [4096, 5120], P('head'), may hold values from -0.09375 to 0.09375
Outputs:
- video_out: bfloat16 [1024, 5120], P(('seq', 'head'))
The draws below stay inside these ranges and needn't reach their ends.
All inputs are finite; a program needn't handle non-finite values.
Results may differ from the reference program's by a relative error of at most 0.018.
Values may be sent and summed in bfloat16 or wider, within the bound.
A program may use at most 128 MiB of HBM per device.

```python
import jax
import jax.numpy as jnp
from jax import lax

D = 5120
HEADS = 32
HD = 128
TEXT = 512
TOKENS = 1024
N_HEAD = 4


def paired_draw(key):
    shape = (TOKENS, HEADS * HD)
    key_rows = jnp.clip(jax.random.normal(jax.random.fold_in(key, 11), shape, jnp.float32), -6.0, 6.0)
    queries = jnp.clip(jax.random.normal(jax.random.fold_in(key, 12), shape, jnp.float32), -6.0, 6.0)
    return (queries, key_rows)


def draw_video_q(key, part):
    queries, key_rows = paired_draw(key)
    return queries.astype(jnp.bfloat16)


def draw_video_k(key, part):
    queries, key_rows = paired_draw(key)
    return key_rows.astype(jnp.bfloat16)


def block_levels(rng, extent, pieces, low, largest):
    def one(position, blocks):
        draws = jax.random.uniform(jax.random.fold_in(jax.random.fold_in(rng, 6), position), (blocks,), jnp.float32, low / len(pieces), largest / len(pieces))
        return jnp.repeat(jnp.exp(draws), extent[position] // blocks).reshape((-1,) + (1,) * (len(extent) - position - 1))

    loudness = one(*pieces[0])
    for cut in pieces[1:]:
        loudness = loudness * one(*cut)
    return loudness


def normal_values(own_key, shape, scale, most, split=(), dtype=jnp.bfloat16):
    values = jax.random.normal(own_key, shape, jnp.float32) * scale
    if len(split) > 0:
        values = block_levels(own_key, shape, split, -0.22, 0.18) * values
    return jnp.clip(values, min=-most, max=most).astype(dtype)


def setup_inputs(seed: int = 0) -> dict:
    arg_keys = jax.random.split(jax.random.key(seed), 7)
    video_q = draw_video_q(jax.random.fold_in(arg_keys[6], 71), 0)
    video_k = draw_video_k(jax.random.fold_in(arg_keys[6], 71), 0)
    video_v = normal_values(arg_keys[2], (TOKENS, HEADS * HD), 1.0, 6.0, ((0, 32),))
    text_k = normal_values(arg_keys[3], (TEXT, HEADS * HD), 1.0, 6.0, ((1, 4),))
    text_v = normal_values(arg_keys[4], (TEXT, HEADS * HD), 1.0, 6.0, ((1, 4),))
    out_weight = normal_values(arg_keys[5], (HEADS * HD, D), (HEADS * HD) ** -0.5, 0.09375, ((0, 4),))
    return {"video_q": video_q, "video_k": video_k, "video_v": video_v, "text_k": text_k, "text_v": text_v, "out_weight": out_weight}


def head_output(operands):
    queries, key_rows, value_rows = operands
    scores = jnp.dot(queries, key_rows.T, preferred_element_type=jnp.float32) * (HD ** -0.5)
    row_max = jnp.max(scores, axis=1, keepdims=True)
    weights = jnp.exp(scores - row_max).astype(jnp.bfloat16)
    totals = jnp.sum(weights.astype(jnp.float32), axis=1, keepdims=True)
    summed = jnp.dot(weights, value_rows, preferred_element_type=jnp.float32)
    return (summed / totals).astype(jnp.bfloat16)


def split_heads(array):
    return array.reshape(array.shape[0], HEADS, HD).transpose(1, 0, 2)


def reference(video_q, video_k, video_v, text_k, text_v, out_weight):
    tokens = video_q.shape[0]
    all_keys = jnp.concatenate([split_heads(video_k), split_heads(text_k)], axis=1)
    all_values = jnp.concatenate([split_heads(video_v), split_heads(text_v)], axis=1)
    attended = lax.map(head_output, (split_heads(video_q), all_keys, all_values))
    attended = attended.transpose(1, 0, 2).reshape(tokens, HEADS * HD)
    group_width = HEADS * HD // N_HEAD
    group_inputs = attended.reshape(tokens, N_HEAD, group_width).transpose(1, 0, 2)
    weight_groups = out_weight.reshape(N_HEAD, group_width, D)

    def add_group(summed_out, operands):
        part_in, part_weight = operands
        partial_out = jnp.dot(part_in, part_weight, preferred_element_type=jnp.float32).astype(jnp.bfloat16)
        partial_out = lax.optimization_barrier(partial_out)
        return summed_out + partial_out.astype(jnp.float32), None

    summed_out, unused = lax.scan(add_group, jnp.zeros((tokens, D), jnp.float32), (group_inputs, weight_groups))
    return summed_out.astype(jnp.bfloat16)
```

```python
import functools
import itertools
import math

import jax
import jax.numpy as jnp
from jax import lax
from jax.experimental import pallas as pl
from jax.experimental.pallas import tpu as pltpu
from jax.sharding import PartitionSpec as P

HD = 128
BF16 = jnp.bfloat16
F32 = jnp.float32
CORES = 2
SIDES = 2
COLUMN = 2
LAG = 2
SCALE = HD ** (-0.5) * math.log2(math.e)


def kernel(
    n_seq, n_head, q_ref, k_ref, v_ref, tk_ref, tv_ref, w_ref, own_ref, pair_ref, far_ref,
    stage, keys_in, vals, queries, tk, tv, w, probs, att_send, stat_send, att, stat_in, mix, merged,
    acc, part, pair_in, y_send,
    load_sem, text_sem, w_sem, k_send, k_recv, v_send, v_recv, q_send, q_recv,
    att_ssem, att_rsem, stat_ssem, stat_rsem, pair_ssem, pair_rsem, y_ssem, y_rsem, own_sem, ready_sem,
):
    s, g = lax.axis_index("seq"), lax.axis_index("head")
    core, chip = lax.rem(g, CORES), lax.div(g, CORES)
    chips = n_head // CORES
    near = n_seq // SIDES
    side, seat = lax.div(s, near), lax.rem(s, near)
    rows, depth = q_ref.shape[0], w_ref.shape[0]
    n_cols = w_sem.shape[0]
    width = w_ref.shape[1] // n_cols
    halves, sub = att.shape[1], att.shape[4]
    wide = tk.shape[1]
    heads = wide // HD
    texts_here = tk.shape[0]
    m = CORES * sub
    split = near * n_head * rows

    def block(n):
        return pl.ds(pl.multiple_of(n * wide, wide), wide)

    def cols(n):
        return pl.ds(n * width, width)

    def part_of(r):
        return pl.ds(r * sub, sub)

    loads = [
        pltpu.make_async_copy(ref, stage.at[i], load_sem.at[i])
        for i, ref in enumerate((k_ref, v_ref, q_ref))
    ]
    my_text = pl.ds(pl.multiple_of(side * texts_here, texts_here), texts_here)
    texts = [
        pltpu.make_async_copy(tk_ref.at[my_text, block(seat)], tk, text_sem.at[0]),
        pltpu.make_async_copy(tv_ref.at[my_text, block(seat)], tv, text_sem.at[1]),
    ]
    weights = [
        pltpu.make_async_copy(w_ref.at[:, cols(n)], w.at[:, cols(n)], w_sem.at[n])
        for n in range(n_cols)
    ]
    for copy in loads + texts + weights:
        copy.start()

    turns = list(range(1, chips)) + [0]
    seat_z, seat_x = lax.div(seat, COLUMN), lax.rem(seat, COLUMN)
    inner = lax.rem(side + seat_z, SIDES) == 1
    outer = jnp.logical_not(inner)

    def device(across, oz, ox, turn, c):
        place = lax.rem(seat_z + oz, near // COLUMN) * COLUMN + lax.rem(seat_x + ox, COLUMN)
        ts = lax.rem(side + across, SIDES) * near + place
        return ts, lax.rem(chip + turn, chips) * CORES + lax.rem(core + c, CORES)

    def hops(across, oz, ox, turn, c):
        flat = ox + (turn > 0)
        if not across:
            return [(flat + oz, None)]
        if oz == 0:
            return [(flat + 2, None)]
        return [(flat + 1, inner), (flat + 3, outer)]

    def under(condition, action):
        if condition is None:
            action()
        else:
            pl.when(condition)(action)

    others = [
        where for where in itertools.product(
            (1, 0), range(near // COLUMN), range(COLUMN), turns, range(CORES)
        ) if any(where)
    ]
    reach = max(far for where in others for far, _ in hops(*where))

    def greet(semaphore, where):
        ts, tg = device(*where)
        pl.semaphore_signal(
            semaphore, inc=1, device_id={"seq": ts, "head": tg},
            device_id_type=pl.DeviceIdType.MESH,
        )

    def greet_adjacent(semaphore, some):
        always, within = 0, 0
        for where in others:
            for far, condition in hops(*where):
                if far <= 1 and some(where):
                    under(condition, functools.partial(greet, semaphore, where))
                    always, within = always + (condition is None), within + (condition is inner)
        pl.semaphore_wait(semaphore, always + jnp.where(inner, within, 0))

    greet_adjacent(pltpu.get_barrier_semaphore(), lambda where: True)

    def send(src, dst, ssem, rsem, ts, tg):
        return pltpu.make_async_remote_copy(
            src_ref=src, dst_ref=dst, send_sem=ssem, recv_sem=rsem,
            device_id={"seq": ts, "head": tg}, device_id_type=pl.DeviceIdType.MESH,
        )

    def wait_for(ref, sem):
        pltpu.make_async_copy(ref, ref, sem).wait()

    def owned(ts, tg):
        return block(tg * near + lax.rem(ts, near))

    mine = owned(s, g)

    def give(i, chosen, dst, ssem, rsem, where):
        ts, tg = device(*where)
        send(stage.at[i, chosen, owned(ts, tg)], dst, ssem, rsem, ts, tg).start()

    def give_query(r, where):
        turn = where[3]
        give(
            2, part_of(r), queries.at[s, g, part_of(r)],
            q_send.at[turn, r], q_recv.at[turn, r], where,
        )

    for copy in loads:
        copy.wait()
    given = set()
    everything = pl.ds(0, rows)
    for known in range(1, reach + 1):
        if known > 1:
            greet_adjacent(ready_sem.at[known - 2], lambda where: where[4] == 0)
        now = [
            (where, condition) for where in others for far, condition in hops(*where)
            if far == known or known == 1 and far == 0
        ]
        for i, (buffer, ssem, rsem) in enumerate(((keys_in, k_send, k_recv), (vals, v_send, v_recv))):
            for where, condition in now:
                if not where[0]:
                    give(i, everything, buffer.at[seat, g], ssem, rsem, where)
        for r in range(halves):
            for where, condition in now:
                if where[3] > 0 or condition is inner:
                    under(condition, functools.partial(give_query, r, where))
                    given.add((r, where, condition is outer))
    for r in range(halves):
        for where in others:
            for far, condition in hops(*where):
                if (r, where, condition is outer) not in given:
                    under(condition, functools.partial(give_query, r, where))
    pltpu.make_async_copy(stage.at[0, :, mine], keys_in.at[seat, g], k_recv).start()
    pltpu.make_async_copy(stage.at[1, :, mine], vals.at[seat, g], v_recv).start()
    for r in range(halves):
        pltpu.make_async_copy(
            stage.at[2, part_of(r), mine], queries.at[s, g, part_of(r)], q_recv.at[0, r]
        ).start()

    for copy in texts:
        copy.wait()
    wait_for(keys_in, k_recv)
    wait_for(vals, v_recv)
    keyed = (((1,), (1,)), ((), ()))
    owners = [(t, lax.rem(chip + t, chips)) for t in turns]
    passes = [(t, owner, r) for t, owner in owners for r in range(halves)]
    count = near * m
    lane = lax.broadcasted_iota(jnp.int32, (count, HD), 1)

    def lanes(h):
        return pl.ds(h * HD, HD)

    def deliver(t, r, c, b):
        here = lax.rem(seat + 1 + b, near)
        pieces = (
            (
                att_send.at[t, r, c, here], att.at[t, r, side, :, :, block(seat)],
                att_ssem.at[t, r], att_rsem.at[t, r, seat],
            ),
            (
                stat_send.at[t, r, c], stat_in.at[t, r, side, seat],
                stat_ssem.at[t, r], stat_rsem.at[t, r, seat],
            ),
        )
        for src, dst, ssem, rsem in pieces:
            if c == SIDES - 1 and b == near - 1:
                pltpu.make_async_copy(src, dst, rsem).start()
            else:
                to_side = lax.rem(side + c + 1, SIDES)
                send(src, dst, ssem, rsem, to_side * near + here, g).start()

    for t, owner, r in passes:
        chosen = pl.ds(owner * CORES, CORES)
        wait_for(queries.at[:, chosen, part_of(r)], q_recv.at[t, r])
        for c in range(SIDES):
            to_side = lax.rem(side + c + 1, SIDES)
            first = to_side * near
            tops = []
            for h in range(heads):
                q = queries[pl.ds(first, near), chosen, part_of(r), lanes(h)].reshape(count, HD)
                keys = keys_in[:, :, :, lanes(h)].reshape(split, HD)
                on_video = lax.dot_general(q, keys, keyed, preferred_element_type=F32)
                on_text = lax.dot_general(q, tk[:, lanes(h)], keyed, preferred_element_type=F32)
                top = jnp.maximum(
                    jnp.max(on_video, axis=1, keepdims=True),
                    jnp.max(on_text, axis=1, keepdims=True),
                )
                probs[c, h, :, :split] = jnp.exp2((on_video - top) * SCALE).astype(BF16)
                probs[c, h, :, split:] = jnp.exp2((on_text - top) * SCALE).astype(BF16)
                tops.append(top)
            logs = None
            for h in range(heads):
                values, words = vals[:, :, :, lanes(h)].reshape(split, HD), tv[:, lanes(h)]
                ahead = jnp.dot(
                    probs[c, h, :, :split],
                    jnp.concatenate([values, jnp.ones_like(values)], axis=1),
                    preferred_element_type=F32,
                ) + jnp.dot(
                    probs[c, h, :, split:],
                    jnp.concatenate([words, jnp.ones_like(words)], axis=1),
                    preferred_element_type=F32,
                )
                total = ahead[:, HD:]
                done = (ahead[:, :HD] / total).astype(BF16)
                att_send[t, r, c, :, :, :, lanes(h)] = done.reshape(near, CORES, sub, HD)
                log = tops[h] * SCALE + jnp.log2(total)
                logs = log if h == 0 else jnp.where(lane < h * (HD // heads), logs, log)
            turned = logs.T
            for h in range(heads):
                at = h * (HD // heads)
                stat_send[t, r, c, h : h + 1, :] = turned[at : at + 1, :]
            if t > 0:
                for b in range(near):
                    deliver(t, r, c, b)
    for b in range(near):
        for r in range(halves):
            for c in range(SIDES):
                deliver(0, r, c, b)

    def merge(t, r, n):
        wait_for(att.at[t, r, :, :, :, block(n)], att_rsem.at[t, r, n])
        wait_for(stat_in.at[t, r, :, n], stat_rsem.at[t, r, n])
        weight = 1.0 / (1.0 + jnp.exp2(stat_in[t, r, 1, n] - stat_in[t, r, 0, n]))
        weight = jnp.concatenate(
            [jnp.broadcast_to(weight[h : h + 1], (HD // heads, count)) for h in range(heads)], axis=0
        ).T
        mix[t, r, n] = weight
        mine = mix[t, r, n, pl.ds(pl.multiple_of(seat * m, m), m), :]
        out = []
        for h in range(heads):
            at = h * (HD // heads)
            held = [
                att[t, r, i, :, :, pl.ds(pl.multiple_of(n * wide + h * HD, HD), HD)]
                .reshape(m, HD).astype(F32)
                for i in range(SIDES)
            ]
            out.append((held[1] + (held[0] - held[1]) * mine[:, at : at + 1]).astype(BF16))
        return jnp.concatenate(out, axis=1)

    def to_pair(t, r, n):
        landing = pair_ref.at[part_of(r), cols(n)] if t == 0 else pair_in.at[t - 1, r, :, cols(n)]
        return send(
            part.at[t, r, 1 - core, :, cols(n)], landing,
            pair_ssem.at[t, r, n], pair_rsem.at[t, r, n], s, g + 1 - 2 * core,
        )

    def to_owner(t, r, owner, n):
        return send(
            y_send.at[t - 1, r, :, cols(n)], far_ref.at[t - 1, part_of(r), cols(n)],
            y_ssem.at[t - 1, r, n], y_rsem.at[t - 1, r, n], s, owner * CORES + core,
        )

    def to_own(r, n):
        return pltpu.make_async_copy(
            part.at[0, r, core, :, cols(n)], own_ref.at[part_of(r), cols(n)], own_sem.at[r, n]
        )

    def cross(t, r, owner, n):
        to_pair(t, r, n).wait_recv()
        total = part[t, r, core, :, cols(n)].astype(F32) + pair_in[t - 1, r, :, cols(n)].astype(F32)
        y_send[t - 1, r, :, cols(n)] = total.astype(BF16)
        to_owner(t, r, owner, n).start()

    pending = []
    for copy in weights:
        copy.wait()
    for t, owner in owners[:-1]:
        for r in range(halves):
            for n in range(near):
                merged[t, r, :, n * wide : (n + 1) * wide] = merge(t, r, n)
            for n in range(n_cols):
                made = jnp.dot(merged[t, r], w[:, cols(n)], preferred_element_type=F32)
                part[t, r, :, :, cols(n)] = made.astype(BF16).reshape(CORES, sub, width)
                to_pair(t, r, n).start()
                pending.append((t, r, owner, n))
                if len(pending) > LAG:
                    cross(*pending.pop(0))
    while pending:
        cross(*pending.pop(0))
    for step in range(near):
        z = lax.rem(seat + 2 * near - 1 - step, near)
        both = jnp.concatenate([merge(0, r, z) for r in range(halves)], axis=0)
        for n in range(n_cols):
            made = jnp.dot(both, w[block(z), cols(n)], preferred_element_type=F32)
            if step > 0:
                made = made + acc[:, cols(n)]
            if step < near - 1:
                acc[:, cols(n)] = made
            else:
                part[0, :, :, :, cols(n)] = made.astype(BF16).reshape(halves, CORES, sub, width)
                for r in range(halves):
                    to_pair(0, r, n).start()
                    to_own(r, n).start()
            if pending:
                cross(*pending.pop(0))
    while pending:
        cross(*pending.pop(0))
    for buffer, sem in ((keys_in, k_send), (vals, v_send)):
        wait_for(buffer.reshape(near * n_head, rows, wide).at[1:], sem)
    for t, owner in owners:
        sent = n_seq * CORES - (t == 0)
        for r in range(halves):
            wait_for(
                queries.reshape(n_seq * n_head, rows, wide).at[:sent, part_of(r)], q_send.at[t, r]
            )
            wait_for(
                att_send.at[t, r].reshape(n_seq, CORES, sub, wide).at[1:], att_ssem.at[t, r]
            )
            wait_for(stat_in.at[t, r].reshape(n_seq, heads, count).at[1:], stat_ssem.at[t, r])
            for n in range(n_cols):
                to_pair(t, r, n).wait_send()
                if t > 0:
                    to_owner(t, r, owner, n).wait()
                else:
                    to_pair(t, r, n).wait_recv()
                    to_own(r, n).wait()


def fused(n_seq, n_head, video_q, video_k, video_v, text_k, text_v, out_weight):
    rows, text = video_q.shape[0], text_k.shape[0]
    depth, d = out_weight.shape
    near = n_seq // SIDES
    wide = text_k.shape[1] // near
    heads = wide // HD
    chips = n_head // CORES
    halves = 2 if rows % 32 == 0 else 1
    sub = rows // halves
    count = near * CORES * sub
    keys = near * n_head * rows + text // SIDES
    n_cols = next(n for n in (4, 5, 8, 2, 1) if d % (n * 2 * HD) == 0)
    anywhere = pl.BlockSpec(memory_space=pl.ANY)
    dma = pltpu.SemaphoreType.DMA
    far = max(chips - 1, 1)
    own, pair, across = pl.pallas_call(
        functools.partial(kernel, n_seq, n_head),
        out_shape=(
            jax.ShapeDtypeStruct((rows, d), BF16),
            jax.ShapeDtypeStruct((rows, d), BF16),
            jax.ShapeDtypeStruct((far, rows, d), BF16),
        ),
        in_specs=[anywhere] * 6,
        out_specs=(anywhere,) * 3,
        scratch_shapes=[
            pltpu.VMEM((3, rows, video_q.shape[1]), BF16),
            pltpu.VMEM((near, n_head, rows, wide), BF16),
            pltpu.VMEM((near, n_head, rows, wide), BF16),
            pltpu.VMEM((n_seq, n_head, rows, wide), BF16),
            pltpu.VMEM((text // SIDES, wide), BF16),
            pltpu.VMEM((text // SIDES, wide), BF16),
            pltpu.VMEM((depth, d), BF16),
            pltpu.VMEM((SIDES, heads, count, keys), BF16),
            pltpu.VMEM((chips, halves, SIDES, near, CORES, sub, wide), BF16),
            pltpu.VMEM((chips, halves, SIDES, heads, count), F32),
            pltpu.VMEM((chips, halves, SIDES, CORES, sub, depth), BF16),
            pltpu.VMEM((chips, halves, SIDES, near, heads, count), F32),
            pltpu.VMEM((chips, halves, near, count, HD), F32),
            pltpu.VMEM((chips, halves, CORES * sub, depth), BF16),
            pltpu.VMEM((rows * CORES, d), F32),
            pltpu.VMEM((chips, halves, CORES, sub, d), BF16),
            pltpu.VMEM((far, halves, sub, d), BF16),
            pltpu.VMEM((far, halves, sub, d), BF16),
            dma((3,)), dma((2,)), dma((n_cols,)),
            dma(()), dma(()), dma(()), dma(()), dma((chips, halves)), dma((chips, halves)),
            dma((chips, halves)), dma((chips, halves, near)),
            dma((chips, halves)), dma((chips, halves, near)),
            dma((chips, halves, n_cols)), dma((chips, halves, n_cols)),
            dma((far, halves, n_cols)), dma((far, halves, n_cols)), dma((halves, n_cols)),
            pltpu.SemaphoreType.REGULAR((n_seq,)),
        ],
        compiler_params=pltpu.CompilerParams(
            collective_id=0, has_side_effects=True, vmem_limit_bytes=60 * 2**20
        ),
    )(video_q, video_k, video_v, text_k, text_v, out_weight)
    total = own.astype(F32) + pair.astype(F32)
    for t in range(chips - 1):
        total = total + across[t].astype(F32)
    return total.astype(BF16)


def as_heads(array):
    return array.reshape(array.shape[0], array.shape[1] // HD, HD)


def scores_of(query_heads, key_heads):
    return jnp.einsum(
        "qhd,khd->hqk", query_heads, key_heads, preferred_element_type=jnp.float32
    ) * HD ** (-0.5)


def weigh_values(scores, row_max, value_heads):
    weights = jnp.exp(scores - row_max[..., None]).astype(jnp.bfloat16)
    totals = jnp.sum(weights.astype(jnp.float32), axis=2)
    summed = jnp.einsum("hqk,khd->hqd", weights, value_heads, preferred_element_type=jnp.float32)
    return (totals, summed)


def local_partial(query_heads, key_heads, value_heads):
    scores = scores_of(query_heads, key_heads)
    row_max = jnp.max(scores, axis=2)
    totals, summed = weigh_values(scores, row_max, value_heads)
    return (row_max, totals, summed)


def combine_partial(first, second):
    joint = jnp.maximum(first[0], second[0])
    first_factor = jnp.exp(first[0] - joint)
    second_factor = jnp.exp(second[0] - joint)
    totals = first[1] * first_factor + second[1] * second_factor
    summed = first[2] * first_factor[..., None] + second[2] * second_factor[..., None]
    return (joint, totals, summed)


def body(video_q, video_k, video_v, text_k, text_v, out_weight):
    queries, key_rows, value_rows = (
        lax.all_to_all(video_q, "head", split_axis=1, concat_axis=0, tiled=True),
        lax.all_to_all(video_k, "head", split_axis=1, concat_axis=0, tiled=True),
        lax.all_to_all(video_v, "head", split_axis=1, concat_axis=0, tiled=True),
    )
    rows_here = queries.shape[0]
    query_heads = as_heads(queries)
    text_part = local_partial(query_heads, as_heads(text_k), as_heads(text_v))
    merged = combine_partial(
        text_part,
        local_partial(
            query_heads,
            as_heads(lax.all_gather(key_rows, "seq", axis=0, tiled=True)),
            as_heads(lax.all_gather(value_rows, "seq", axis=0, tiled=True)),
        ),
    )
    normalized = merged[2] / merged[1][..., None]
    attended = normalized.transpose(1, 0, 2).reshape(rows_here, -1).astype(jnp.bfloat16)
    return lax.psum_scatter(
        jnp.dot(attended, out_weight, preferred_element_type=jnp.float32).astype(jnp.bfloat16),
        "head",
        scatter_dimension=0,
        tiled=True,
    )


def solution(mesh):
    n_seq, n_head = mesh.shape["seq"], mesh.shape["head"]

    def step(*arrays):
        heads_here = arrays[3].shape[1] // HD
        paired = heads_here == n_seq and n_head % CORES == 0 and n_head == 2 * CORES and n_seq == 2 * SIDES * COLUMN
        tiled = n_seq // SIDES * CORES * arrays[0].shape[0] == 2 * HD
        return fused(n_seq, n_head, *arrays) if paired and tiled else body(*arrays)

    in_specs = (
        P(("seq", "head"), None),
        P(("seq", "head"), None),
        P(("seq", "head"), None),
        P(None, "head"),
        P(None, "head"),
        P("head", None),
    )
    out_specs = P(("seq", "head"), None)
    return jax.shard_map(step, mesh=mesh, in_specs=in_specs, out_specs=out_specs, check_vma=False)
```

```python
import functools
import itertools
import math

import jax
import jax.numpy as jnp
from jax import lax
from jax.experimental import pallas as pl
from jax.experimental.pallas import tpu as pltpu
from jax.sharding import PartitionSpec as P

HD = 128
BF16 = jnp.bfloat16
F32 = jnp.float32
CORES = 2
SIDES = 2
COLUMN = 2
LAG = 2
SCALE = HD ** (-0.5) * math.log2(math.e)


def kernel(
    n_seq, n_head, q_ref, k_ref, v_ref, tk_ref, tv_ref, w_ref, own_ref, pair_ref, far_ref,
    stage, keys_in, vals, queries, tk, tv, w, probs, att_send, stat_send, att, stat_in, mix, merged,
    acc, part, pair_in, y_send,
    load_sem, text_sem, w_sem, k_send, k_recv, v_send, v_recv, q_send, q_recv,
    att_ssem, att_rsem, stat_ssem, stat_rsem, pair_ssem, pair_rsem, y_ssem, y_rsem, own_sem, ready_sem,
):
    s, g = lax.axis_index("seq"), lax.axis_index("head")
    core, chip = lax.rem(g, CORES), lax.div(g, CORES)
    chips = n_head // CORES
    near = n_seq // SIDES
    side, seat = lax.div(s, near), lax.rem(s, near)
    rows, depth = q_ref.shape[0], w_ref.shape[0]
    n_cols = w_sem.shape[0]
    width = w_ref.shape[1] // n_cols
    halves, sub = att.shape[1], att.shape[4]
    wide = tk.shape[1]
    heads = wide // HD
    texts_here = tk.shape[0]
    m = CORES * sub
    split = near * n_head * rows

    def block(n):
        return pl.ds(pl.multiple_of(n * wide, wide), wide)

    def cols(n):
        return pl.ds(n * width, width)

    def part_of(r):
        return pl.ds(r * sub, sub)

    loads = [
        pltpu.make_async_copy(ref, stage.at[i], load_sem.at[i])
        for i, ref in enumerate((k_ref, v_ref, q_ref))
    ]
    my_text = pl.ds(pl.multiple_of(side * texts_here, texts_here), texts_here)
    texts = [
        pltpu.make_async_copy(tk_ref.at[my_text, block(seat)], tk, text_sem.at[0]),
        pltpu.make_async_copy(tv_ref.at[my_text, block(seat)], tv, text_sem.at[1]),
    ]
    weights = [
        pltpu.make_async_copy(w_ref.at[:, cols(n)], w.at[:, cols(n)], w_sem.at[n])
        for n in range(n_cols)
    ]
    for copy in loads + texts + weights:
        copy.start()

    turns = list(range(1, chips)) + [0]
    seat_z, seat_x = lax.div(seat, COLUMN), lax.rem(seat, COLUMN)
    inner = lax.rem(side + seat_z, SIDES) == 1
    outer = jnp.logical_not(inner)

    def device(across, oz, ox, turn, c):
        place = lax.rem(seat_z + oz, near // COLUMN) * COLUMN + lax.rem(seat_x + ox, COLUMN)
        ts = lax.rem(side + across, SIDES) * near + place
        return ts, lax.rem(chip + turn, chips) * CORES + lax.rem(core + c, CORES)

    def hops(across, oz, ox, turn, c):
        flat = ox + (turn > 0)
        if not across:
            return [(flat + oz, None)]
        if oz == 0:
            return [(flat + 2, None)]
        return [(flat + 1, inner), (flat + 3, outer)]

    def under(condition, action):
        if condition is None:
            action()
        else:
            pl.when(condition)(action)

    others = [
        where for where in itertools.product(
            (1, 0), range(near // COLUMN), range(COLUMN), turns, range(CORES)
        ) if any(where)
    ]
    reach = max(far for where in others for far, _ in hops(*where))

    def greet(semaphore, where):
        ts, tg = device(*where)
        pl.semaphore_signal(
            semaphore, inc=1, device_id={"seq": ts, "head": tg},
            device_id_type=pl.DeviceIdType.MESH,
        )

    def greet_adjacent(semaphore, some):
        always, within = 0, 0
        for where in others:
            for far, condition in hops(*where):
                if far <= 1 and some(where):
                    under(condition, functools.partial(greet, semaphore, where))
                    always, within = always + (condition is None), within + (condition is inner)
        pl.semaphore_wait(semaphore, always + jnp.where(inner, within, 0))

    greet_adjacent(pltpu.get_barrier_semaphore(), lambda where: True)

    def send(src, dst, ssem, rsem, ts, tg):
        return pltpu.make_async_remote_copy(
            src_ref=src, dst_ref=dst, send_sem=ssem, recv_sem=rsem,
            device_id={"seq": ts, "head": tg}, device_id_type=pl.DeviceIdType.MESH,
        )

    def wait_for(ref, sem):
        pltpu.make_async_copy(ref, ref, sem).wait()

    def owned(ts, tg):
        return block(tg * near + lax.rem(ts, near))

    mine = owned(s, g)

    def give(i, chosen, dst, ssem, rsem, where):
        ts, tg = device(*where)
        send(stage.at[i, chosen, owned(ts, tg)], dst, ssem, rsem, ts, tg).start()

    def give_query(r, where):
        turn = where[3]
        give(
            2, part_of(r), queries.at[s, g, part_of(r)],
            q_send.at[turn, r], q_recv.at[turn, r], where,
        )

    for copy in loads:
        copy.wait()
    given = set()
    everything = pl.ds(0, rows)
    for known in range(1, reach + 1):
        if known > 1:
            greet_adjacent(ready_sem.at[known - 2], lambda where: where[4] == 0)
        now = [
            (where, condition) for where in others for far, condition in hops(*where)
            if far == known or known == 1 and far == 0
        ]
        for where, condition in now:
            if not where[0]:
                give(0, everything, keys_in.at[seat, g], k_send, k_recv, where)
                give(1, everything, vals.at[seat, g], v_send, v_recv, where)
        for r in range(halves):
            for where, condition in now:
                if condition is inner:
                    under(condition, functools.partial(give_query, r, where))
                    given.add((r, where, condition is outer))
    urgent = [(r, where) for r in range(halves) for where in others if where[3] > 0]
    others_last = [(r, where) for where in others for r in range(halves) if where[3] == 0]
    for r, where in urgent + others_last:
        for far, condition in hops(*where):
            if (r, where, condition is outer) not in given:
                under(condition, functools.partial(give_query, r, where))
    pltpu.make_async_copy(stage.at[0, :, mine], keys_in.at[seat, g], k_recv).start()
    pltpu.make_async_copy(stage.at[1, :, mine], vals.at[seat, g], v_recv).start()
    for r in range(halves):
        pltpu.make_async_copy(
            stage.at[2, part_of(r), mine], queries.at[s, g, part_of(r)], q_recv.at[0, r]
        ).start()

    for copy in texts:
        copy.wait()
    wait_for(keys_in, k_recv)
    wait_for(vals, v_recv)
    keyed = (((1,), (1,)), ((), ()))
    owners = [(t, lax.rem(chip + t, chips)) for t in turns]
    passes = [(t, owner, r) for t, owner in owners for r in range(halves)]
    count = near * m
    lane = lax.broadcasted_iota(jnp.int32, (count, HD), 1)

    def lanes(h):
        return pl.ds(h * HD, HD)

    def deliver(t, r, c, b):
        here = lax.rem(seat + 1 + b, near)
        pieces = (
            (
                att_send.at[t, r, c, here], att.at[t, r, side, :, :, block(seat)],
                att_ssem.at[t, r], att_rsem.at[t, r, seat],
            ),
            (
                stat_send.at[t, r, c], stat_in.at[t, r, side, seat],
                stat_ssem.at[t, r], stat_rsem.at[t, r, seat],
            ),
        )
        for src, dst, ssem, rsem in pieces:
            if c == SIDES - 1 and b == near - 1:
                pltpu.make_async_copy(src, dst, rsem).start()
            else:
                to_side = lax.rem(side + c + 1, SIDES)
                send(src, dst, ssem, rsem, to_side * near + here, g).start()

    for t, owner, r in passes:
        chosen = pl.ds(owner * CORES, CORES)
        wait_for(queries.at[:, chosen, part_of(r)], q_recv.at[t, r])
        for c in range(SIDES):
            to_side = lax.rem(side + c + 1, SIDES)
            first = to_side * near
            tops = []
            for h in range(heads):
                q = queries[pl.ds(first, near), chosen, part_of(r), lanes(h)].reshape(count, HD)
                keys = keys_in[:, :, :, lanes(h)].reshape(split, HD)
                on_video = lax.dot_general(q, keys, keyed, preferred_element_type=F32)
                on_text = lax.dot_general(q, tk[:, lanes(h)], keyed, preferred_element_type=F32)
                top = jnp.maximum(
                    jnp.max(on_video, axis=1, keepdims=True),
                    jnp.max(on_text, axis=1, keepdims=True),
                )
                probs[c, h, :, :split] = jnp.exp2((on_video - top) * SCALE).astype(BF16)
                probs[c, h, :, split:] = jnp.exp2((on_text - top) * SCALE).astype(BF16)
                tops.append(top)
            logs = None
            for h in range(heads):
                values, words = vals[:, :, :, lanes(h)].reshape(split, HD), tv[:, lanes(h)]
                ahead = jnp.dot(
                    probs[c, h, :, :split],
                    jnp.concatenate([values, jnp.ones_like(values)], axis=1),
                    preferred_element_type=F32,
                ) + jnp.dot(
                    probs[c, h, :, split:],
                    jnp.concatenate([words, jnp.ones_like(words)], axis=1),
                    preferred_element_type=F32,
                )
                total = ahead[:, HD:]
                done = (ahead[:, :HD] / total).astype(BF16)
                att_send[t, r, c, :, :, :, lanes(h)] = done.reshape(near, CORES, sub, HD)
                log = tops[h] * SCALE + jnp.log2(total)
                logs = log if h == 0 else jnp.where(lane < h * (HD // heads), logs, log)
            turned = logs.T
            for h in range(heads):
                at = h * (HD // heads)
                stat_send[t, r, c, h : h + 1, :] = turned[at : at + 1, :]
            if t > 0:
                for b in range(near):
                    deliver(t, r, c, b)
    for b in range(near):
        for r in range(halves):
            for c in range(SIDES):
                deliver(0, r, c, b)

    def merge(t, r, n):
        wait_for(att.at[t, r, :, :, :, block(n)], att_rsem.at[t, r, n])
        wait_for(stat_in.at[t, r, :, n], stat_rsem.at[t, r, n])
        weight = 1.0 / (1.0 + jnp.exp2(stat_in[t, r, 1, n] - stat_in[t, r, 0, n]))
        weight = jnp.concatenate(
            [jnp.broadcast_to(weight[h : h + 1], (HD // heads, count)) for h in range(heads)], axis=0
        ).T
        mix[t, r, n] = weight
        mine = mix[t, r, n, pl.ds(pl.multiple_of(seat * m, m), m), :]
        out = []
        for h in range(heads):
            at = h * (HD // heads)
            held = [
                att[t, r, i, :, :, pl.ds(pl.multiple_of(n * wide + h * HD, HD), HD)]
                .reshape(m, HD).astype(F32)
                for i in range(SIDES)
            ]
            out.append((held[1] + (held[0] - held[1]) * mine[:, at : at + 1]).astype(BF16))
        return jnp.concatenate(out, axis=1)

    def to_pair(t, r, n):
        landing = pair_ref.at[part_of(r), cols(n)] if t == 0 else pair_in.at[t - 1, r, :, cols(n)]
        return send(
            part.at[t, r, 1 - core, :, cols(n)], landing,
            pair_ssem.at[t, r, n], pair_rsem.at[t, r, n], s, g + 1 - 2 * core,
        )

    def to_owner(t, r, owner, n):
        return send(
            y_send.at[t - 1, r, :, cols(n)], far_ref.at[t - 1, part_of(r), cols(n)],
            y_ssem.at[t - 1, r, n], y_rsem.at[t - 1, r, n], s, owner * CORES + core,
        )

    def to_own(r, n):
        return pltpu.make_async_copy(
            part.at[0, r, core, :, cols(n)], own_ref.at[part_of(r), cols(n)], own_sem.at[r, n]
        )

    def cross(t, r, owner, n):
        to_pair(t, r, n).wait_recv()
        total = part[t, r, core, :, cols(n)].astype(F32) + pair_in[t - 1, r, :, cols(n)].astype(F32)
        y_send[t - 1, r, :, cols(n)] = total.astype(BF16)
        to_owner(t, r, owner, n).start()

    pending = []
    for copy in weights:
        copy.wait()
    for t, owner in owners[:-1]:
        for r in range(halves):
            for n in range(near):
                merged[t, r, :, n * wide : (n + 1) * wide] = merge(t, r, n)
            for n in range(n_cols):
                made = jnp.dot(merged[t, r], w[:, cols(n)], preferred_element_type=F32)
                part[t, r, :, :, cols(n)] = made.astype(BF16).reshape(CORES, sub, width)
                to_pair(t, r, n).start()
                pending.append((t, r, owner, n))
                if len(pending) > LAG:
                    cross(*pending.pop(0))
    while pending:
        cross(*pending.pop(0))
    for step in range(near):
        z = lax.rem(seat + 2 * near - 1 - step, near)
        both = jnp.concatenate([merge(0, r, z) for r in range(halves)], axis=0)
        for n in range(n_cols):
            made = jnp.dot(both, w[block(z), cols(n)], preferred_element_type=F32)
            if step > 0:
                made = made + acc[:, cols(n)]
            if step < near - 1:
                acc[:, cols(n)] = made
            else:
                part[0, :, :, :, cols(n)] = made.astype(BF16).reshape(halves, CORES, sub, width)
                for r in range(halves):
                    to_pair(0, r, n).start()
                    to_own(r, n).start()
            if pending:
                cross(*pending.pop(0))
    while pending:
        cross(*pending.pop(0))
    for buffer, sem in ((keys_in, k_send), (vals, v_send)):
        wait_for(buffer.reshape(near * n_head, rows, wide).at[1:], sem)
    for t, owner in owners:
        sent = n_seq * CORES - (t == 0)
        for r in range(halves):
            wait_for(
                queries.reshape(n_seq * n_head, rows, wide).at[:sent, part_of(r)], q_send.at[t, r]
            )
            wait_for(
                att_send.at[t, r].reshape(n_seq, CORES, sub, wide).at[1:], att_ssem.at[t, r]
            )
            wait_for(stat_in.at[t, r].reshape(n_seq, heads, count).at[1:], stat_ssem.at[t, r])
            for n in range(n_cols):
                to_pair(t, r, n).wait_send()
                if t > 0:
                    to_owner(t, r, owner, n).wait()
                else:
                    to_pair(t, r, n).wait_recv()
                    to_own(r, n).wait()


def fused(n_seq, n_head, video_q, video_k, video_v, text_k, text_v, out_weight):
    rows, text = video_q.shape[0], text_k.shape[0]
    depth, d = out_weight.shape
    near = n_seq // SIDES
    wide = text_k.shape[1] // near
    heads = wide // HD
    chips = n_head // CORES
    halves = 2 if rows % 32 == 0 else 1
    sub = rows // halves
    count = near * CORES * sub
    keys = near * n_head * rows + text // SIDES
    n_cols = next(n for n in (4, 5, 8, 2, 1) if d % (n * 2 * HD) == 0)
    anywhere = pl.BlockSpec(memory_space=pl.ANY)
    dma = pltpu.SemaphoreType.DMA
    far = max(chips - 1, 1)
    own, pair, across = pl.pallas_call(
        functools.partial(kernel, n_seq, n_head),
        out_shape=(
            jax.ShapeDtypeStruct((rows, d), BF16),
            jax.ShapeDtypeStruct((rows, d), BF16),
            jax.ShapeDtypeStruct((far, rows, d), BF16),
        ),
        in_specs=[anywhere] * 6,
        out_specs=(anywhere,) * 3,
        scratch_shapes=[
            pltpu.VMEM((3, rows, video_q.shape[1]), BF16),
            pltpu.VMEM((near, n_head, rows, wide), BF16),
            pltpu.VMEM((near, n_head, rows, wide), BF16),
            pltpu.VMEM((n_seq, n_head, rows, wide), BF16),
            pltpu.VMEM((text // SIDES, wide), BF16),
            pltpu.VMEM((text // SIDES, wide), BF16),
            pltpu.VMEM((depth, d), BF16),
            pltpu.VMEM((SIDES, heads, count, keys), BF16),
            pltpu.VMEM((chips, halves, SIDES, near, CORES, sub, wide), BF16),
            pltpu.VMEM((chips, halves, SIDES, heads, count), F32),
            pltpu.VMEM((chips, halves, SIDES, CORES, sub, depth), BF16),
            pltpu.VMEM((chips, halves, SIDES, near, heads, count), F32),
            pltpu.VMEM((chips, halves, near, count, HD), F32),
            pltpu.VMEM((chips, halves, CORES * sub, depth), BF16),
            pltpu.VMEM((rows * CORES, d), F32),
            pltpu.VMEM((chips, halves, CORES, sub, d), BF16),
            pltpu.VMEM((far, halves, sub, d), BF16),
            pltpu.VMEM((far, halves, sub, d), BF16),
            dma((3,)), dma((2,)), dma((n_cols,)),
            dma(()), dma(()), dma(()), dma(()), dma((chips, halves)), dma((chips, halves)),
            dma((chips, halves)), dma((chips, halves, near)),
            dma((chips, halves)), dma((chips, halves, near)),
            dma((chips, halves, n_cols)), dma((chips, halves, n_cols)),
            dma((far, halves, n_cols)), dma((far, halves, n_cols)), dma((halves, n_cols)),
            pltpu.SemaphoreType.REGULAR((n_seq,)),
        ],
        compiler_params=pltpu.CompilerParams(
            collective_id=0, has_side_effects=True, vmem_limit_bytes=60 * 2**20
        ),
    )(video_q, video_k, video_v, text_k, text_v, out_weight)
    total = own.astype(F32) + pair.astype(F32)
    for t in range(chips - 1):
        total = total + across[t].astype(F32)
    return total.astype(BF16)


def as_heads(array):
    return array.reshape(array.shape[0], array.shape[1] // HD, HD)


def scores_of(query_heads, key_heads):
    return jnp.einsum(
        "qhd,khd->hqk", query_heads, key_heads, preferred_element_type=jnp.float32
    ) * HD ** (-0.5)


def weigh_values(scores, row_max, value_heads):
    weights = jnp.exp(scores - row_max[..., None]).astype(jnp.bfloat16)
    totals = jnp.sum(weights.astype(jnp.float32), axis=2)
    summed = jnp.einsum("hqk,khd->hqd", weights, value_heads, preferred_element_type=jnp.float32)
    return (totals, summed)


def local_partial(query_heads, key_heads, value_heads):
    scores = scores_of(query_heads, key_heads)
    row_max = jnp.max(scores, axis=2)
    totals, summed = weigh_values(scores, row_max, value_heads)
    return (row_max, totals, summed)


def combine_partial(first, second):
    joint = jnp.maximum(first[0], second[0])
    first_factor = jnp.exp(first[0] - joint)
    second_factor = jnp.exp(second[0] - joint)
    totals = first[1] * first_factor + second[1] * second_factor
    summed = first[2] * first_factor[..., None] + second[2] * second_factor[..., None]
    return (joint, totals, summed)


def body(video_q, video_k, video_v, text_k, text_v, out_weight):
    queries, key_rows, value_rows = (
        lax.all_to_all(video_q, "head", split_axis=1, concat_axis=0, tiled=True),
        lax.all_to_all(video_k, "head", split_axis=1, concat_axis=0, tiled=True),
        lax.all_to_all(video_v, "head", split_axis=1, concat_axis=0, tiled=True),
    )
    rows_here = queries.shape[0]
    query_heads = as_heads(queries)
    text_part = local_partial(query_heads, as_heads(text_k), as_heads(text_v))
    merged = combine_partial(
        text_part,
        local_partial(
            query_heads,
            as_heads(lax.all_gather(key_rows, "seq", axis=0, tiled=True)),
            as_heads(lax.all_gather(value_rows, "seq", axis=0, tiled=True)),
        ),
    )
    normalized = merged[2] / merged[1][..., None]
    attended = normalized.transpose(1, 0, 2).reshape(rows_here, -1).astype(jnp.bfloat16)
    return lax.psum_scatter(
        jnp.dot(attended, out_weight, preferred_element_type=jnp.float32).astype(jnp.bfloat16),
        "head",
        scatter_dimension=0,
        tiled=True,
    )


def solution(mesh):
    n_seq, n_head = mesh.shape["seq"], mesh.shape["head"]

    def step(*arrays):
        heads_here = arrays[3].shape[1] // HD
        paired = heads_here == n_seq and n_head % CORES == 0 and n_head == 2 * CORES and n_seq == 2 * SIDES * COLUMN
        tiled = n_seq // SIDES * CORES * arrays[0].shape[0] == 2 * HD
        return fused(n_seq, n_head, *arrays) if paired and tiled else body(*arrays)

    in_specs = (
        P(("seq", "head"), None),
        P(("seq", "head"), None),
        P(("seq", "head"), None),
        P(None, "head"),
        P(None, "head"),
        P("head", None),
    )
    out_specs = P(("seq", "head"), None)
    return jax.shard_map(step, mesh=mesh, in_specs=in_specs, out_specs=out_specs, check_vma=False)
```

```python
import functools
import itertools
import math

import jax
import jax.numpy as jnp
from jax import lax
from jax.experimental import pallas as pl
from jax.experimental.pallas import tpu as pltpu
from jax.sharding import PartitionSpec as P

HD = 128
BF16 = jnp.bfloat16
F32 = jnp.float32
CORES = 2
SIDES = 2
COLUMN = 2
LAG = 2
SCALE = HD ** (-0.5) * math.log2(math.e)


def kernel(
    n_seq, n_head, q_ref, k_ref, v_ref, tk_ref, tv_ref, w_ref, own_ref, pair_ref, far_ref,
    stage, keys_in, vals, queries, tk, tv, w, probs, att_send, stat_send, att, stat_in, mix, merged,
    acc, part, pair_in, y_send,
    load_sem, text_sem, w_sem, k_send, k_recv, v_send, v_recv, q_send, q_recv,
    att_ssem, att_rsem, stat_ssem, stat_rsem, pair_ssem, pair_rsem, y_ssem, y_rsem, own_sem, ready_sem,
):
    s, g = lax.axis_index("seq"), lax.axis_index("head")
    core, chip = lax.rem(g, CORES), lax.div(g, CORES)
    chips = n_head // CORES
    near = n_seq // SIDES
    side, seat = lax.div(s, near), lax.rem(s, near)
    rows, depth = q_ref.shape[0], w_ref.shape[0]
    n_cols = w_sem.shape[0]
    width = w_ref.shape[1] // n_cols
    halves, sub = att.shape[1], att.shape[4]
    wide = tk.shape[1]
    heads = wide // HD
    texts_here = tk.shape[0]
    m = CORES * sub
    split = near * n_head * rows

    def block(n):
        return pl.ds(pl.multiple_of(n * wide, wide), wide)

    def cols(n):
        return pl.ds(n * width, width)

    def part_of(r):
        return pl.ds(r * sub, sub)

    loads = [
        pltpu.make_async_copy(ref, stage.at[i], load_sem.at[i])
        for i, ref in enumerate((k_ref, v_ref, q_ref))
    ]
    my_text = pl.ds(pl.multiple_of(side * texts_here, texts_here), texts_here)
    texts = [
        pltpu.make_async_copy(tk_ref.at[my_text, block(seat)], tk, text_sem.at[0]),
        pltpu.make_async_copy(tv_ref.at[my_text, block(seat)], tv, text_sem.at[1]),
    ]
    weights = [
        pltpu.make_async_copy(w_ref.at[:, cols(n)], w.at[:, cols(n)], w_sem.at[n])
        for n in range(n_cols)
    ]
    for copy in loads + texts + weights:
        copy.start()

    turns = list(range(1, chips)) + [0]
    seat_z, seat_x = lax.div(seat, COLUMN), lax.rem(seat, COLUMN)
    inner = lax.rem(side + seat_z, SIDES) == 1
    outer = jnp.logical_not(inner)

    def device(across, oz, ox, turn, c):
        place = lax.rem(seat_z + oz, near // COLUMN) * COLUMN + lax.rem(seat_x + ox, COLUMN)
        ts = lax.rem(side + across, SIDES) * near + place
        return ts, lax.rem(chip + turn, chips) * CORES + lax.rem(core + c, CORES)

    def hops(across, oz, ox, turn, c):
        flat = ox + (turn > 0)
        if not across:
            return [(flat + oz, None)]
        if oz == 0:
            return [(flat + 2, None)]
        return [(flat + 1, inner), (flat + 3, outer)]

    def under(condition, action):
        if condition is None:
            action()
        else:
            pl.when(condition)(action)

    others = [
        where for where in itertools.product(
            (1, 0), range(near // COLUMN), range(COLUMN), turns, range(CORES)
        ) if any(where)
    ]
    reach = max(far for where in others for far, _ in hops(*where))

    def greet(semaphore, where):
        ts, tg = device(*where)
        pl.semaphore_signal(
            semaphore, inc=1, device_id={"seq": ts, "head": tg},
            device_id_type=pl.DeviceIdType.MESH,
        )

    def greet_adjacent(semaphore, some):
        always, within = 0, 0
        for where in others:
            for far, condition in hops(*where):
                if far <= 1 and some(where):
                    under(condition, functools.partial(greet, semaphore, where))
                    always, within = always + (condition is None), within + (condition is inner)
        pl.semaphore_wait(semaphore, always + jnp.where(inner, within, 0))

    greet_adjacent(pltpu.get_barrier_semaphore(), lambda where: True)

    def send(src, dst, ssem, rsem, ts, tg):
        return pltpu.make_async_remote_copy(
            src_ref=src, dst_ref=dst, send_sem=ssem, recv_sem=rsem,
            device_id={"seq": ts, "head": tg}, device_id_type=pl.DeviceIdType.MESH,
        )

    def wait_for(ref, sem):
        pltpu.make_async_copy(ref, ref, sem).wait()

    def owned(ts, tg):
        return block(tg * near + lax.rem(ts, near))

    mine = owned(s, g)

    def give(i, chosen, dst, ssem, rsem, where):
        ts, tg = device(*where)
        send(stage.at[i, chosen, owned(ts, tg)], dst, ssem, rsem, ts, tg).start()

    def give_query(r, where):
        turn = where[3]
        give(
            2, part_of(r), queries.at[s, g, part_of(r)],
            q_send.at[turn, r], q_recv.at[turn, r], where,
        )

    for copy in loads:
        copy.wait()
    given = set()
    everything = pl.ds(0, rows)
    for known in range(1, reach + 1):
        if known > 1:
            greet_adjacent(ready_sem.at[known - 2], lambda where: where[4] == 0)
        now = [
            (where, condition) for where in others for far, condition in hops(*where)
            if far == known or known == 1 and far == 0
        ]
        for where, condition in now:
            if not where[0]:
                give(0, everything, keys_in.at[seat, g], k_send, k_recv, where)
                give(1, everything, vals.at[seat, g], v_send, v_recv, where)
        for r in range(halves):
            for where, condition in now:
                if condition is inner:
                    under(condition, functools.partial(give_query, r, where))
                    given.add((r, where, condition is outer))
    urgent = [(r, where) for r in range(halves) for where in others if where[3] > 0]
    others_last = [(r, where) for where in others for r in range(halves) if where[3] == 0]
    for r, where in urgent + others_last:
        for far, condition in hops(*where):
            if (r, where, condition is outer) not in given:
                under(condition, functools.partial(give_query, r, where))
    pltpu.make_async_copy(stage.at[0, :, mine], keys_in.at[seat, g], k_recv).start()
    pltpu.make_async_copy(stage.at[1, :, mine], vals.at[seat, g], v_recv).start()
    for r in range(halves):
        pltpu.make_async_copy(
            stage.at[2, part_of(r), mine], queries.at[s, g, part_of(r)], q_recv.at[0, r]
        ).start()

    for copy in texts:
        copy.wait()
    wait_for(keys_in, k_recv)
    wait_for(vals, v_recv)
    keyed = (((1,), (1,)), ((), ()))
    owners = [(t, lax.rem(chip + t, chips)) for t in turns]
    passes = [(t, owner, r) for t, owner in owners for r in range(halves)]
    count = near * m
    lane = lax.broadcasted_iota(jnp.int32, (count, HD), 1)

    def lanes(h):
        return pl.ds(h * HD, HD)

    def deliver(t, r, c, b):
        here = lax.rem(seat + 1 + b, near)
        pieces = (
            (
                att_send.at[t, r, c, here], att.at[t, r, side, :, :, block(seat)],
                att_ssem.at[t, r], att_rsem.at[t, r, seat],
            ),
            (
                stat_send.at[t, r, c], stat_in.at[t, r, side, seat],
                stat_ssem.at[t, r], stat_rsem.at[t, r, seat],
            ),
        )
        for src, dst, ssem, rsem in pieces[::-1]:
            if c == SIDES - 1 and b == near - 1:
                pltpu.make_async_copy(src, dst, rsem).start()
            else:
                to_side = lax.rem(side + c + 1, SIDES)
                parts = [(src.at[e], dst.at[e]) for e in range(CORES)] if len(src.shape) == 3 else [(src, dst)]
                for one, other in parts:
                    send(one, other, ssem, rsem, to_side * near + here, g).start()

    for t, owner, r in passes:
        chosen = pl.ds(owner * CORES, CORES)
        wait_for(queries.at[:, chosen, part_of(r)], q_recv.at[t, r])
        for c in range(SIDES):
            to_side = lax.rem(side + c + 1, SIDES)
            first = to_side * near
            tops = []
            for h in range(heads):
                q = queries[pl.ds(first, near), chosen, part_of(r), lanes(h)].reshape(count, HD)
                keys = keys_in[:, :, :, lanes(h)].reshape(split, HD)
                on_video = lax.dot_general(q, keys, keyed, preferred_element_type=F32)
                on_text = lax.dot_general(q, tk[:, lanes(h)], keyed, preferred_element_type=F32)
                top = jnp.maximum(
                    jnp.max(on_video, axis=1, keepdims=True),
                    jnp.max(on_text, axis=1, keepdims=True),
                )
                probs[c, h, :, :split] = jnp.exp2((on_video - top) * SCALE).astype(BF16)
                probs[c, h, :, split:] = jnp.exp2((on_text - top) * SCALE).astype(BF16)
                tops.append(top)
            logs = None
            for h in range(heads):
                values, words = vals[:, :, :, lanes(h)].reshape(split, HD), tv[:, lanes(h)]
                ahead = jnp.dot(
                    probs[c, h, :, :split],
                    jnp.concatenate([values, jnp.ones_like(values)], axis=1),
                    preferred_element_type=F32,
                ) + jnp.dot(
                    probs[c, h, :, split:],
                    jnp.concatenate([words, jnp.ones_like(words)], axis=1),
                    preferred_element_type=F32,
                )
                total = ahead[:, HD:]
                done = (ahead[:, :HD] / total).astype(BF16)
                att_send[t, r, c, :, :, :, lanes(h)] = done.reshape(near, CORES, sub, HD)
                log = tops[h] * SCALE + jnp.log2(total)
                logs = log if h == 0 else jnp.where(lane < h * (HD // heads), logs, log)
            turned = logs.T
            for h in range(heads):
                at = h * (HD // heads)
                stat_send[t, r, c, h : h + 1, :] = turned[at : at + 1, :]
            if t > 0:
                for b in range(near):
                    deliver(t, r, c, b)
    for b in range(near):
        for r in range(halves):
            for c in range(SIDES):
                deliver(0, r, c, b)

    def merge(t, r, n):
        wait_for(att.at[t, r, :, :, :, block(n)], att_rsem.at[t, r, n])
        wait_for(stat_in.at[t, r, :, n], stat_rsem.at[t, r, n])
        weight = 1.0 / (1.0 + jnp.exp2(stat_in[t, r, 1, n] - stat_in[t, r, 0, n]))
        weight = jnp.concatenate(
            [jnp.broadcast_to(weight[h : h + 1], (HD // heads, count)) for h in range(heads)], axis=0
        ).T
        mix[t, r, n] = weight
        mine = mix[t, r, n, pl.ds(pl.multiple_of(seat * m, m), m), :]
        out = []
        for h in range(heads):
            at = h * (HD // heads)
            held = [
                att[t, r, i, :, :, pl.ds(pl.multiple_of(n * wide + h * HD, HD), HD)]
                .reshape(m, HD).astype(F32)
                for i in range(SIDES)
            ]
            out.append((held[1] + (held[0] - held[1]) * mine[:, at : at + 1]).astype(BF16))
        return jnp.concatenate(out, axis=1)

    def to_pair(t, r, n):
        landing = pair_ref.at[part_of(r), cols(n)] if t == 0 else pair_in.at[t - 1, r, :, cols(n)]
        return send(
            part.at[t, r, 1 - core, :, cols(n)], landing,
            pair_ssem.at[t, r, n], pair_rsem.at[t, r, n], s, g + 1 - 2 * core,
        )

    def to_owner(t, r, owner, n):
        return send(
            y_send.at[t - 1, r, :, cols(n)], far_ref.at[t - 1, part_of(r), cols(n)],
            y_ssem.at[t - 1, r, n], y_rsem.at[t - 1, r, n], s, owner * CORES + core,
        )

    def to_own(r, n):
        return pltpu.make_async_copy(
            part.at[0, r, core, :, cols(n)], own_ref.at[part_of(r), cols(n)], own_sem.at[r, n]
        )

    def cross(t, r, owner, n):
        to_pair(t, r, n).wait_recv()
        total = part[t, r, core, :, cols(n)].astype(F32) + pair_in[t - 1, r, :, cols(n)].astype(F32)
        y_send[t - 1, r, :, cols(n)] = total.astype(BF16)
        to_owner(t, r, owner, n).start()

    pending = []
    for copy in weights:
        copy.wait()
    for t, owner in owners[:-1]:
        for r in range(halves):
            for n in range(near):
                merged[t, r, :, n * wide : (n + 1) * wide] = merge(t, r, n)
            for n in range(n_cols):
                made = jnp.dot(merged[t, r], w[:, cols(n)], preferred_element_type=F32)
                part[t, r, :, :, cols(n)] = made.astype(BF16).reshape(CORES, sub, width)
                to_pair(t, r, n).start()
                pending.append((t, r, owner, n))
                if len(pending) > LAG:
                    cross(*pending.pop(0))
    while pending:
        cross(*pending.pop(0))
    for step in range(near):
        z = lax.rem(seat + 2 * near - 1 - step, near)
        both = jnp.concatenate([merge(0, r, z) for r in range(halves)], axis=0)
        for n in range(n_cols):
            made = jnp.dot(both, w[block(z), cols(n)], preferred_element_type=F32)
            if step > 0:
                made = made + acc[:, cols(n)]
            if step < near - 1:
                acc[:, cols(n)] = made
            else:
                part[0, :, :, :, cols(n)] = made.astype(BF16).reshape(halves, CORES, sub, width)
                for r in range(halves):
                    to_pair(0, r, n).start()
                    to_own(r, n).start()
            if pending:
                cross(*pending.pop(0))
    while pending:
        cross(*pending.pop(0))
    for buffer, sem in ((keys_in, k_send), (vals, v_send)):
        wait_for(buffer.reshape(near * n_head, rows, wide).at[1:], sem)
    for t, owner in owners:
        sent = n_seq * CORES - (t == 0)
        for r in range(halves):
            wait_for(
                queries.reshape(n_seq * n_head, rows, wide).at[:sent, part_of(r)], q_send.at[t, r]
            )
            wait_for(
                att_send.at[t, r].reshape(n_seq, CORES, sub, wide).at[1:], att_ssem.at[t, r]
            )
            wait_for(stat_in.at[t, r].reshape(n_seq, heads, count).at[1:], stat_ssem.at[t, r])
            for n in range(n_cols):
                to_pair(t, r, n).wait_send()
                if t > 0:
                    to_owner(t, r, owner, n).wait()
                else:
                    to_pair(t, r, n).wait_recv()
                    to_own(r, n).wait()


def fused(n_seq, n_head, video_q, video_k, video_v, text_k, text_v, out_weight):
    rows, text = video_q.shape[0], text_k.shape[0]
    depth, d = out_weight.shape
    near = n_seq // SIDES
    wide = text_k.shape[1] // near
    heads = wide // HD
    chips = n_head // CORES
    halves = 2 if rows % 32 == 0 else 1
    sub = rows // halves
    count = near * CORES * sub
    keys = near * n_head * rows + text // SIDES
    n_cols = next(n for n in (4, 5, 8, 2, 1) if d % (n * 2 * HD) == 0)
    anywhere = pl.BlockSpec(memory_space=pl.ANY)
    dma = pltpu.SemaphoreType.DMA
    far = max(chips - 1, 1)
    own, pair, across = pl.pallas_call(
        functools.partial(kernel, n_seq, n_head),
        out_shape=(
            jax.ShapeDtypeStruct((rows, d), BF16),
            jax.ShapeDtypeStruct((rows, d), BF16),
            jax.ShapeDtypeStruct((far, rows, d), BF16),
        ),
        in_specs=[anywhere] * 6,
        out_specs=(anywhere,) * 3,
        scratch_shapes=[
            pltpu.VMEM((3, rows, video_q.shape[1]), BF16),
            pltpu.VMEM((near, n_head, rows, wide), BF16),
            pltpu.VMEM((near, n_head, rows, wide), BF16),
            pltpu.VMEM((n_seq, n_head, rows, wide), BF16),
            pltpu.VMEM((text // SIDES, wide), BF16),
            pltpu.VMEM((text // SIDES, wide), BF16),
            pltpu.VMEM((depth, d), BF16),
            pltpu.VMEM((SIDES, heads, count, keys), BF16),
            pltpu.VMEM((chips, halves, SIDES, near, CORES, sub, wide), BF16),
            pltpu.VMEM((chips, halves, SIDES, heads, count), F32),
            pltpu.VMEM((chips, halves, SIDES, CORES, sub, depth), BF16),
            pltpu.VMEM((chips, halves, SIDES, near, heads, count), F32),
            pltpu.VMEM((chips, halves, near, count, HD), F32),
            pltpu.VMEM((chips, halves, CORES * sub, depth), BF16),
            pltpu.VMEM((rows * CORES, d), F32),
            pltpu.VMEM((chips, halves, CORES, sub, d), BF16),
            pltpu.VMEM((far, halves, sub, d), BF16),
            pltpu.VMEM((far, halves, sub, d), BF16),
            dma((3,)), dma((2,)), dma((n_cols,)),
            dma(()), dma(()), dma(()), dma(()), dma((chips, halves)), dma((chips, halves)),
            dma((chips, halves)), dma((chips, halves, near)),
            dma((chips, halves)), dma((chips, halves, near)),
            dma((chips, halves, n_cols)), dma((chips, halves, n_cols)),
            dma((far, halves, n_cols)), dma((far, halves, n_cols)), dma((halves, n_cols)),
            pltpu.SemaphoreType.REGULAR((n_seq,)),
        ],
        compiler_params=pltpu.CompilerParams(
            collective_id=0, has_side_effects=True, vmem_limit_bytes=60 * 2**20
        ),
    )(video_q, video_k, video_v, text_k, text_v, out_weight)
    total = own.astype(F32) + pair.astype(F32)
    for t in range(chips - 1):
        total = total + across[t].astype(F32)
    return total.astype(BF16)


def as_heads(array):
    return array.reshape(array.shape[0], array.shape[1] // HD, HD)


def scores_of(query_heads, key_heads):
    return jnp.einsum(
        "qhd,khd->hqk", query_heads, key_heads, preferred_element_type=jnp.float32
    ) * HD ** (-0.5)


def weigh_values(scores, row_max, value_heads):
    weights = jnp.exp(scores - row_max[..., None]).astype(jnp.bfloat16)
    totals = jnp.sum(weights.astype(jnp.float32), axis=2)
    summed = jnp.einsum("hqk,khd->hqd", weights, value_heads, preferred_element_type=jnp.float32)
    return (totals, summed)


def local_partial(query_heads, key_heads, value_heads):
    scores = scores_of(query_heads, key_heads)
    row_max = jnp.max(scores, axis=2)
    totals, summed = weigh_values(scores, row_max, value_heads)
    return (row_max, totals, summed)


def combine_partial(first, second):
    joint = jnp.maximum(first[0], second[0])
    first_factor = jnp.exp(first[0] - joint)
    second_factor = jnp.exp(second[0] - joint)
    totals = first[1] * first_factor + second[1] * second_factor
    summed = first[2] * first_factor[..., None] + second[2] * second_factor[..., None]
    return (joint, totals, summed)


def body(video_q, video_k, video_v, text_k, text_v, out_weight):
    queries, key_rows, value_rows = (
        lax.all_to_all(video_q, "head", split_axis=1, concat_axis=0, tiled=True),
        lax.all_to_all(video_k, "head", split_axis=1, concat_axis=0, tiled=True),
        lax.all_to_all(video_v, "head", split_axis=1, concat_axis=0, tiled=True),
    )
    rows_here = queries.shape[0]
    query_heads = as_heads(queries)
    text_part = local_partial(query_heads, as_heads(text_k), as_heads(text_v))
    merged = combine_partial(
        text_part,
        local_partial(
            query_heads,
            as_heads(lax.all_gather(key_rows, "seq", axis=0, tiled=True)),
            as_heads(lax.all_gather(value_rows, "seq", axis=0, tiled=True)),
        ),
    )
    normalized = merged[2] / merged[1][..., None]
    attended = normalized.transpose(1, 0, 2).reshape(rows_here, -1).astype(jnp.bfloat16)
    return lax.psum_scatter(
        jnp.dot(attended, out_weight, preferred_element_type=jnp.float32).astype(jnp.bfloat16),
        "head",
        scatter_dimension=0,
        tiled=True,
    )


def solution(mesh):
    n_seq, n_head = mesh.shape["seq"], mesh.shape["head"]

    def step(*arrays):
        heads_here = arrays[3].shape[1] // HD
        paired = heads_here == n_seq and n_head % CORES == 0 and n_head == 2 * CORES and n_seq == 2 * SIDES * COLUMN
        tiled = n_seq // SIDES * CORES * arrays[0].shape[0] == 2 * HD
        return fused(n_seq, n_head, *arrays) if paired and tiled else body(*arrays)

    in_specs = (
        P(("seq", "head"), None),
        P(("seq", "head"), None),
        P(("seq", "head"), None),
        P(None, "head"),
        P(None, "head"),
        P("head", None),
    )
    out_specs = P(("seq", "head"), None)
    return jax.shard_map(step, mesh=mesh, in_specs=in_specs, out_specs=out_specs, check_vma=False)
```
